32 devices in a mesh: prompt: 4 (over y, core), span: 8 (over z, x).
Axes of the slice: x: 2, y: 2, z: 4, core: 2. Of those that a mesh axis runs over, the one named last changes fastest.
Arguments:
- queries: bfloat16 [32, 8, 8192], P('prompt', 'span'), may hold values from -40 to 40
- query_pos: int32 [32, 8], P('prompt', 'span'), may hold values from 2 to 4095
- fresh_keys: bfloat16 [32, 8, 1024], P('prompt', 'span'), may hold values from -20 to 20
- fresh_values: bfloat16 [32, 8, 1024], P('prompt', 'span'), may hold values from -6 to 6
- cache_keys: bfloat16 [4, 8, 512, 1024], P('prompt', 'span'), may hold values from -18 to 18
- cache_values: bfloat16 [4, 8, 512, 1024], P('prompt', 'span'), may hold values from -6 to 6
- block_len: int32 [4, 8], P('prompt', 'span'), may hold values from 128 to 512
- block_owner: int32 [8, 32, 1], P('span', 'prompt'), may hold values from 0 to 3; in each aligned block of 8 rows (0 to 7, 8 to 15, ..., all dimensions but the last counted through in order) at most 4 rows name the same one
Outputs:
- attended: bfloat16 [32, 8, 8192], P('prompt', 'span')
The draws below stay inside these ranges and needn't reach their ends.
Inputs may be any that keep to these rules, and one draw needn't show every extreme that they name: `block_owner`: among the 8 prompts of one device, at most 4 name the same stored passage for one passage position.
All inputs are finite; a program needn't handle non-finite values.
Results may differ from the reference program's by a relative error of at most 0.01.
Values may be sent and summed in bfloat16 or wider, within the bound.
A program may use at most 128 MiB of HBM per device.

```python
import math
import jax
import jax.numpy as jnp
import numpy as np
from jax import lax

H = 64
KVH = 8
HD = 128
PR_DEV = 8
CL = 512
PROMPTS = 32
SEL = 8
CTX = 4096
MOST = 4
N_PROMPT = 4
N_SPAN = 8


def query_table(key):
    queries = jnp.clip(jax.random.normal(jax.random.fold_in(key, 12), (PROMPTS, SEL, H, HD), jnp.float32), -6.0, 6.0)
    return queries


def draw_queries(key, part):
    queries = query_table(key)
    return jnp.clip(queries, -40.0, 40.0).reshape(PROMPTS, SEL, H * HD).astype(jnp.bfloat16)


def draw_fresh_keys(key, part):
    queries = query_table(key)
    group_size = H // KVH
    coupling = 10.0 * group_size / math.sqrt(HD)
    grouped = jnp.mean(queries.reshape(PROMPTS, SEL, KVH, group_size, HD), axis=3)
    noise = jax.random.normal(jax.random.fold_in(key, 13), (PROMPTS, SEL, KVH, HD), jnp.float32)
    fresh = coupling * grouped + noise
    return jnp.clip(fresh, -20.0, 20.0).reshape(PROMPTS, SEL, KVH * HD).astype(jnp.bfloat16)


def draw_cache_keys(key, part):
    stored = 3.0 * jax.random.normal(jax.random.fold_in(key, 14), (N_PROMPT, N_SPAN, CL, KVH * HD), jnp.float32)
    stored = jnp.clip(stored, -18.0, 18.0)
    return stored.astype(jnp.bfloat16)


def set_ends(values, own_key, least, largest):
    extent = values.shape
    index_at = [jax.random.randint(jax.random.fold_in(own_key, axis), (), 0, extent[axis]) for axis in range(len(extent))]
    values = values.at[tuple(index_at)].set(least)
    longest = extent.index(max(extent))
    index_at[longest] = (index_at[longest] + 1) % extent[longest]
    return values.at[tuple(index_at)].set(largest)


def level_of(own_key, dims, pieces, least, high):
    def one(position, shards_of):
        draws = jax.random.uniform(jax.random.fold_in(jax.random.fold_in(own_key, 6), position), (shards_of,), jnp.float32, least / len(pieces), high / len(pieces))
        return jnp.repeat(jnp.exp(draws), dims[position] // shards_of).reshape((-1,) + (1,) * (len(dims) - position - 1))

    factor_of = one(*pieces[0])
    for cut in pieces[1:]:
        factor_of = factor_of * one(*cut)
    return factor_of


def routed_block(rng, own, number, rows, amount, top, limit, slope):
    order = jax.random.permutation(rng, amount)
    heavy_load, usual = load_shares(amount, rows * top, limit, slope, True), load_shares(amount, rows * top, limit, slope, False)
    places = jnp.arange(amount)

    def named(tallies, turn):
        used = int((tallies > 0).sum())
        fixed = max(1, used // 4)
        moved = fixed + (places - fixed + turn * (used - fixed)) % max(1, amount - fixed)
        return jnp.zeros((amount,), jnp.int32).at[order[jnp.where(places < fixed, places, moved)]].set(jnp.asarray(tallies, jnp.int32))

    tallies = jnp.where(number % 4 == 0, named(heavy_load, number // 4), named(usual, number - number // 4 - 1))
    mixed = jax.random.permutation(jax.random.fold_in(own, 3), amount)
    source_of, taker = mixed[0:amount // 2 * 2:2], mixed[1:amount // 2 * 2:2]
    room = jnp.minimum(tallies[source_of] - 1, limit - tallies[taker]) // 2
    room = jnp.where((source_of == order[0]) | (taker == order[0]) | (tallies[taker] == 0), 0, jnp.maximum(room, 0))
    moved = jax.random.randint(jax.random.fold_in(own, 4), (amount // 2,), 0, 1 << 20) % (room + 1)
    tallies = tallies.at[source_of].add(-moved).at[taker].add(moved)
    members = jnp.searchsorted(jnp.cumsum(tallies), jnp.arange(rows * top), side="right").astype(jnp.int32)
    table = members.reshape(top, rows).T
    table = table[jax.random.permutation(jax.random.fold_in(own, 1), rows)]
    turn = jax.random.randint(jax.random.fold_in(own, 2), (rows, 1), 0, top)
    return jnp.take_along_axis(table, (jnp.arange(top)[None, :] + turn) % top, axis=1)


def load_shares(amount, total, limit, slope, full):
    loads = [(1 << 20) // math.isqrt(rank ** slope) + 1 for rank in range(1, amount + 1)]
    largest = limit if full else min(limit, max(-(-total // amount), total * loads[0] // sum(loads)))
    least = 1 if total - largest >= amount - 1 else 0
    counts, rest = [largest] + [least] * (amount - 1), total - largest - least * (amount - 1)
    while rest > 0:
        candidates = [i for i in range(1, amount) if counts[i] < largest] or [i for i in range(1, amount) if counts[i] < limit]
        mass, remaining = sum([loads[i] for i in candidates]), rest
        for i in candidates:
            extra = min(limit - counts[i], max(1, remaining * loads[i] // mass), rest)
            counts[i] = counts[i] + extra
            rest = rest - extra
    return np.array(counts)


def normal_values(stream_key, dims, width, bound, shards=(), kind=jnp.bfloat16):
    factor_of = level_of(stream_key, dims, shards, -0.22, 0.18) if shards else 1.0
    result = jax.random.normal(stream_key, dims, jnp.float32) * width * factor_of
    return jnp.minimum(jnp.maximum(result, -bound), bound).astype(kind)


def setup_inputs(seed: int = 0) -> dict:
    streams_of = jax.random.split(jax.random.key(seed), 9)
    queries = draw_queries(jax.random.fold_in(streams_of[8], 71), 0)
    query_pos = set_ends(jax.random.randint(streams_of[1], (PROMPTS, SEL), 2, CTX), jax.random.fold_in(streams_of[1], 1), 2, CTX - 1).astype(jnp.int32)
    fresh_keys = draw_fresh_keys(jax.random.fold_in(streams_of[8], 71), 0)
    fresh_values = normal_values(streams_of[3], (PROMPTS, SEL, KVH * HD), 1.0, 6.0, ((0, 4), (1, 8)))
    cache_keys = draw_cache_keys(jax.random.fold_in(streams_of[8], 71), 0)
    cache_values = normal_values(streams_of[5], (N_PROMPT, N_SPAN, CL, KVH * HD), 1.0, 6.0, ((0, 4), (1, 8)))
    block_len = set_ends(jax.random.randint(streams_of[6], (N_PROMPT, N_SPAN), CL // 4, CL + 1), jax.random.fold_in(streams_of[6], 1), CL // 4, CL).astype(jnp.int32)
    block_owner_keys = jax.random.split(jax.random.fold_in(streams_of[7], 1), N_SPAN * PROMPTS // PR_DEV)
    block_owner_turns = jax.random.permutation(jax.random.fold_in(streams_of[7], 3), N_SPAN * PROMPTS // PR_DEV)
    block_owner = jax.vmap(lambda own, number: routed_block(jax.random.fold_in(streams_of[7], 2), own, number, PR_DEV, N_PROMPT, 1, MOST, 2))(block_owner_keys, block_owner_turns).reshape((N_SPAN, PROMPTS, 1))
    return {"queries": queries, "query_pos": query_pos, "fresh_keys": fresh_keys, "fresh_values": fresh_values, "cache_keys": cache_keys, "cache_values": cache_values, "block_len": block_len, "block_owner": block_owner}


NEGATIVE = -1e+30

def attend(q_rows, pos_rows, key_rows, values, length, col_start):
    row_count = q_rows.shape[0]
    group_size = H // KVH
    q_heads = q_rows.astype(jnp.float32).reshape(row_count, KVH, group_size, HD)
    k_heads = key_rows.astype(jnp.float32).reshape(-1, KVH, HD)
    v_heads = values.astype(jnp.float32).reshape(-1, KVH, HD)
    slot_ids = jnp.arange(k_heads.shape[0], dtype=jnp.int32)
    usable = (slot_ids[None, :] < length) & (col_start + slot_ids[None, :] < pos_rows[:, None])
    scores = jnp.einsum('rgxd,tgd->rgxt', q_heads, k_heads, precision=lax.Precision.HIGHEST) / math.sqrt(HD)
    visible = usable[:, None, None, :]
    maxima = lax.optimization_barrier(jnp.max(jnp.where(visible, scores, NEGATIVE), axis=-1)).astype(jnp.bfloat16)
    maxima = lax.optimization_barrier(maxima).astype(jnp.float32)
    weights = jnp.where(visible, jnp.exp(scores - maxima[..., None]), 0.0)
    totals = lax.optimization_barrier(jnp.sum(weights, axis=-1)).astype(jnp.bfloat16)
    rounded = lax.optimization_barrier(weights.astype(jnp.bfloat16)).astype(jnp.float32)
    mixture = jnp.einsum('rgxt,tgd->rgxd', rounded, v_heads, precision=lax.Precision.HIGHEST)
    mixture = mixture.astype(jnp.bfloat16).reshape(row_count, H * HD)
    return (mixture, maxima.reshape(row_count, H), totals.reshape(row_count, H))

def reference(queries, query_pos, fresh_keys, fresh_values, cache_keys, cache_values, block_len, block_owner):
    group_size = H // KVH

    def one_prompt(prompt_id):
        q_rows = queries[prompt_id]
        pos_rows = query_pos[prompt_id]

        def one_column(column):
            owner_row = block_owner[column, prompt_id, 0]
            return attend(q_rows, pos_rows, cache_keys[owner_row, column], cache_values[owner_row, column], block_len[owner_row, column], column * CL)
        outputs, maxima, totals = lax.map(one_column, jnp.arange(N_SPAN, dtype=jnp.int32))
        maxima = maxima.astype(jnp.float32)
        totals = totals.astype(jnp.float32)
        q_heads = q_rows.astype(jnp.float32).reshape(SEL, KVH, group_size, HD)
        k_heads = fresh_keys[prompt_id].astype(jnp.float32).reshape(SEL, KVH, HD)
        own_score = jnp.einsum('sgxd,sgd->sgx', q_heads, k_heads, precision=lax.Precision.HIGHEST)
        own_score = own_score.reshape(SEL, H) / math.sqrt(HD)
        own_value = jnp.broadcast_to(fresh_values[prompt_id].astype(jnp.float32).reshape(SEL, KVH, 1, HD), (SEL, KVH, group_size, HD)).reshape(SEL, H, HD)
        highest = jnp.maximum(lax.optimization_barrier(jnp.max(maxima, axis=0)), own_score)
        scale = jnp.exp(maxima - highest[None])
        fresh_scale = jnp.exp(own_score - highest)
        denom = lax.optimization_barrier(jnp.sum(scale * totals, axis=0)) + fresh_scale
        numer = lax.optimization_barrier(jnp.sum(outputs.astype(jnp.float32).reshape(N_SPAN, SEL, H, HD) * scale[..., None], axis=0))
        numer = numer + fresh_scale[..., None] * own_value
        return (numer / denom[..., None]).reshape(SEL, H * HD).astype(jnp.bfloat16)
    return lax.map(one_prompt, jnp.arange(PROMPTS, dtype=jnp.int32))
```

```python
import functools
import math

import jax
import jax.numpy as jnp
from jax import lax
from jax.experimental import pallas as pl
from jax.experimental.pallas import tpu as pltpu
from jax.sharding import PartitionSpec as P

H = 64
KVH = 8
HD = 128
XH = H // KVH
NEGATIVE = -1e30
MESH = pl.DeviceIdType.MESH
CORES = 2


def kernel(
    np_, ns, prompts, slots,
    owner_ref, q_ref, pos_ref, fk_ref, fv_ref, k_ref, v_ref, len_ref,
    out_ref,
    q_all, pos_all, len_all, part, part_all, stat, stat_all, own_ref,
    q_send, q_recv, pos_send, pos_recv, len_send, len_recv,
    load_sem, kvy_send, kvy_recv, kvp_send, kvp_recv,
    part_send, part_recv, stat_send, stat_recv, keep_sem, own_sem,
    *kv,
):
    row = lax.axis_index("prompt")
    col = lax.axis_index("span")
    rows_y = np_ // CORES
    core = lax.rem(row, CORES)
    partner = row + 1 - 2 * core

    def wait_bytes(ref, sem):
        pltpu.make_async_copy(ref, ref, sem).wait()

    def send(src, dst, send_sem, recv_sem, p_, s_):
        pltpu.make_async_remote_copy(
            src_ref=src, dst_ref=dst, send_sem=send_sem, recv_sem=recv_sem,
            device_id=(p_, s_), device_id_type=MESH,
        ).start()

    span_peers = [lax.rem(col + d, ns) for d in range(1, ns)]
    row_peers = [lax.rem(row + d, np_) for d in range(1, np_)]
    y_peers = [lax.rem(row + CORES * d, np_) for d in range(1, rows_y)]

    loads = []
    for g in range(KVH):
        cols = pl.ds(g * HD, HD)
        for i, src in enumerate((k_ref, v_ref)):
            c = pltpu.make_async_copy(
                src.at[:, cols], kv[g].at[row, i], load_sem.at[g, i]
            )
            c.start()
            loads.append(c)
    q_keep = pltpu.make_async_copy(q_ref, q_all.at[col], own_sem.at[0])
    q_keep.start()
    pos_keep = pltpu.make_async_copy(pos_ref, pos_all.at[col], own_sem.at[1])
    pos_keep.start()
    len_keep = pltpu.make_async_copy(len_ref, len_all.at[row], own_sem.at[2])
    len_keep.start()

    barrier = pltpu.get_barrier_semaphore()
    for s in span_peers:
        pl.semaphore_signal(barrier, inc=1, device_id=(row, s), device_id_type=MESH)
    for r in row_peers:
        pl.semaphore_signal(barrier, inc=1, device_id=(r, col), device_id_type=MESH)
    pl.semaphore_wait(barrier, ns - 1 + np_ - 1)

    for r in row_peers:
        send(len_ref, len_all.at[row], len_send, len_recv, r, col)
    for s in span_peers:
        send(pos_ref, pos_all.at[col], pos_send, pos_recv, row, s)
    for g in range(KVH):
        loads[2 * g].wait()
        loads[2 * g + 1].wait()
        for r in y_peers:
            send(kv[g].at[row], kv[g].at[row], kvy_send.at[g], kvy_recv.at[g], r, col)
        send(kv[g].at[row], kv[g].at[row], kvp_send.at[g], kvp_recv.at[g], partner, col)
        for s in span_peers:
            send(q_ref.at[g], q_all.at[col, g], q_send.at[g], q_recv.at[g], row, s)

    lane = lax.broadcasted_iota(jnp.int32, (XH, HD), 1)
    own_ref[...] = jnp.zeros_like(own_ref)
    stat[...] = jnp.zeros_like(stat)

    def own_body(p, carry):
        keys = fk_ref[p].astype(jnp.float32)
        tile = own_ref[...]
        for g in range(KVH):
            q8 = q_ref[g, p].astype(jnp.float32)
            dot = jnp.sum(q8 * keys[g : g + 1], axis=1, keepdims=True)
            tile = jnp.where(lane == g * prompts + p, dot * (1.0 / math.sqrt(HD)), tile)
        own_ref[...] = tile
        return carry

    lax.fori_loop(0, prompts, own_body, 0)

    q_keep.wait()
    pos_keep.wait()
    len_keep.wait()
    wait_bytes(len_all.at[pl.ds(0, np_ - 1)], len_recv)
    wait_bytes(pos_all.at[pl.ds(0, ns - 1)], pos_recv)

    count = ns * XH
    slot_ids = lax.broadcasted_iota(jnp.int32, (count, slots), 1)
    lanes3 = lax.broadcasted_iota(jnp.int32, (ns, XH, HD), 2)
    start = col * slots
    step = 2 if prompts % 2 == 0 else 1

    for g in range(KVH):
        wait_bytes(q_all.at[pl.ds(0, ns - 1), g], q_recv.at[g])
        if rows_y > 1:
            wait_bytes(kv[g].at[pl.ds(0, rows_y - 1)], kvy_recv.at[g])
        for r in y_peers:
            send(kv[g].at[r], kv[g].at[r], kvp_send.at[g], kvp_recv.at[g], partner, col)
        wait_bytes(kv[g].at[pl.ds(0, rows_y)], kvp_recv.at[g])

        def one(p, g=g):
            o = owner_ref[p]
            q64 = q_all[:, g, p].astype(jnp.float32).reshape(count, HD).astype(jnp.bfloat16)
            keys = kv[g][o, 0]
            values = kv[g][o, 1]
            pos3 = jnp.broadcast_to(pos_all[:, pl.ds(p, 1), :], (ns, XH, HD))
            len3 = jnp.broadcast_to(len_all[o][None], (ns, XH, HD))
            limit = jnp.minimum(len3, pos3 - start).reshape(count, HD)
            limit = jnp.concatenate([limit] * (slots // HD), axis=1)
            visible = slot_ids < limit
            scores = lax.dot_general(
                q64, keys, (((1,), (1,)), ((), ())), preferred_element_type=jnp.float32
            ) * (1.0 / math.sqrt(HD))
            scores = jnp.where(visible, scores, NEGATIVE)
            top = jnp.max(scores, axis=1, keepdims=True)
            top = top.astype(jnp.bfloat16).astype(jnp.float32)
            weights = jnp.where(visible, jnp.exp(scores - top), 0.0)
            total = jnp.sum(weights, axis=1, keepdims=True)
            mix = jnp.dot(
                weights.astype(jnp.bfloat16), values, preferred_element_type=jnp.float32
            )
            part[:, g, p] = mix.reshape(ns, XH, HD).astype(jnp.bfloat16)
            here = lanes3 == g * prompts + p
            top3 = jnp.broadcast_to(top, (count, HD)).reshape(ns, XH, HD)
            total3 = jnp.broadcast_to(total, (count, HD)).reshape(ns, XH, HD)
            stat[:, 0] = jnp.where(here, top3, stat[:, 0])
            stat[:, 1] = jnp.where(here, total3, stat[:, 1])

        def body(i, carry):
            for k in range(step):
                one(i * step + k)
            return carry

        lax.fori_loop(0, prompts // step, body, 0)
        for s in span_peers:
            send(part.at[s, g], part_all.at[col, g], part_send.at[g], part_recv.at[g], row, s)
        pltpu.make_async_copy(part.at[col, g], part_all.at[col, g], keep_sem.at[g]).start()

    for s in span_peers:
        send(stat.at[s], stat_all.at[col], stat_send, stat_recv, row, s)
    pltpu.make_async_copy(stat.at[col], stat_all.at[col], own_sem.at[3]).start()

    wait_bytes(stat.at[col], own_sem.at[3])
    wait_bytes(stat_all.at[pl.ds(0, ns - 1)], stat_recv)
    tops = [stat_all[j, 0] for j in range(ns)]
    own = own_ref[...]
    high = own
    for t in tops:
        high = jnp.maximum(high, t)
    own_w = jnp.exp(own - high)
    factors = [jnp.exp(t - high) for t in tops]
    denom = own_w
    for j in range(ns):
        denom = denom + factors[j] * stat_all[j, 1]
    inv = 1.0 / denom
    for j in range(ns):
        stat_all[j, 0] = factors[j] * inv
    own_ref[...] = own_w * inv

    for g in range(KVH):
        wait_bytes(part.at[col, g], keep_sem.at[g])
        wait_bytes(part_all.at[pl.ds(0, ns - 1), g], part_recv.at[g])

    def combine(p, carry):
        shift = lax.rem(HD - p, HD)
        own_s = pltpu.roll(own_ref[...], shift, 1)
        fresh = fv_ref[p].astype(jnp.float32)
        sums = []
        for g in range(KVH):
            lo = g * prompts
            sums.append(own_s[:, lo : lo + 1] * fresh[g : g + 1])
        for j in range(ns):
            f = pltpu.roll(stat_all[j, 0], shift, 1)
            for g in range(KVH):
                lo = g * prompts
                sums[g] = sums[g] + f[:, lo : lo + 1] * part_all[j, g, p].astype(jnp.float32)
        for g in range(KVH):
            out_ref[p, g] = sums[g].astype(jnp.bfloat16)
        return carry

    lax.fori_loop(0, prompts, combine, 0)

    wait_bytes(len_all.at[pl.ds(0, np_ - 1)], len_send)
    wait_bytes(pos_all.at[pl.ds(0, ns - 1)], pos_send)
    wait_bytes(stat_all.at[pl.ds(0, ns - 1)], stat_send)
    for g in range(KVH):
        wait_bytes(q_all.at[pl.ds(0, ns - 1), g], q_send.at[g])
        if rows_y > 1:
            wait_bytes(kv[g].at[pl.ds(0, rows_y - 1)], kvy_send.at[g])
        wait_bytes(kv[g].at[pl.ds(0, rows_y)], kvp_send.at[g])
        wait_bytes(part_all.at[pl.ds(0, ns - 1), g], part_send.at[g])


def on_device(
    queries, query_pos, fresh_keys, fresh_values, cache_keys, cache_values, block_len, block_owner
):
    prompts = queries.shape[0]
    slots = cache_keys.shape[2]
    np_ = lax.axis_size("prompt")
    ns = lax.axis_size("span")
    q = jnp.transpose(queries.reshape(prompts, KVH, XH, HD), (1, 0, 2, 3))
    pos = jnp.broadcast_to(query_pos.reshape(prompts, 1), (prompts, HD))
    lens = jnp.broadcast_to(block_len.reshape(1, 1), (XH, HD))
    owner = block_owner.reshape(prompts)
    vmem = pl.BlockSpec(memory_space=pltpu.VMEM)
    hbm = pl.BlockSpec(memory_space=pl.ANY)
    dma = pltpu.SemaphoreType.DMA
    bf16, f32, i32 = jnp.bfloat16, jnp.float32, jnp.int32
    out = pl.pallas_call(
        functools.partial(kernel, np_, ns, prompts, slots),
        out_shape=jax.ShapeDtypeStruct((prompts, KVH, XH, HD), bf16),
        in_specs=[pl.BlockSpec(memory_space=pltpu.SMEM)] + [vmem] * 4 + [hbm] * 2 + [vmem],
        out_specs=vmem,
        scratch_shapes=[
            pltpu.VMEM((ns, KVH, prompts, XH, HD), bf16),
            pltpu.VMEM((ns, prompts, HD), i32),
            pltpu.VMEM((np_, XH, HD), i32),
            pltpu.VMEM((ns, KVH, prompts, XH, HD), bf16),
            pltpu.VMEM((ns, KVH, prompts, XH, HD), bf16),
            pltpu.VMEM((ns, 2, XH, HD), f32),
            pltpu.VMEM((ns, 2, XH, HD), f32),
            pltpu.VMEM((XH, HD), f32),
            dma((KVH,)), dma((KVH,)), dma, dma, dma, dma,
            dma((KVH, 2)), dma((KVH,)), dma((KVH,)), dma((KVH,)), dma((KVH,)),
            dma((KVH,)), dma((KVH,)), dma, dma, dma((KVH,)), dma((4,)),
        ]
        + [pltpu.VMEM((np_, 2, slots, HD), bf16)] * KVH,
        compiler_params=pltpu.CompilerParams(
            collective_id=0, has_side_effects=True, vmem_limit_bytes=60 * 1024 * 1024
        ),
    )(
        owner,
        q,
        pos,
        fresh_keys.reshape(prompts, KVH, HD),
        fresh_values.reshape(prompts, KVH, HD),
        cache_keys.reshape(slots, KVH * HD),
        cache_values.reshape(slots, KVH * HD),
        lens,
    )
    return out.reshape(prompts, 1, H * HD)


def solution(mesh):
    return jax.shard_map(
        on_device,
        mesh=mesh,
        in_specs=(
            P("prompt", "span", None),
            P("prompt", "span"),
            P("prompt", "span", None),
            P("prompt", "span", None),
            P("prompt", "span", None, None),
            P("prompt", "span", None, None),
            P("prompt", "span"),
            P("span", "prompt", None),
        ),
        out_specs=P("prompt", "span", None),
        check_vma=False,
    )
```

```python
import functools
import math

import jax
import jax.numpy as jnp
from jax import lax
from jax.experimental import pallas as pl
from jax.experimental.pallas import tpu as pltpu
from jax.sharding import PartitionSpec as P

H = 64
KVH = 8
HD = 128
XH = H // KVH
NEGATIVE = -1e30
MESH = pl.DeviceIdType.MESH
CORES = 2


def kernel(
    np_, ns, prompts, slots,
    owner_ref, pos_in, len_in, q_in, fk_in, fv_in, k_ref, v_ref,
    out_ref,
    q_ref, pos_ref, len_ref, fk_ref, fv_ref,
    q_all, pos_all, len_all, part, part_all, stat, stat_all, own_ref,
    q_send, q_recv, pos_send, pos_recv, len_send, len_recv,
    load_sem, kvy_send, kvy_recv, kvp_send, kvp_recv,
    part_send, part_recv, stat_send, stat_recv, keep_sem, own_sem,
    *kv,
):
    row = lax.axis_index("prompt")
    col = lax.axis_index("span")
    rows_y = np_ // CORES
    core = lax.rem(row, CORES)
    partner = row + 1 - 2 * core

    def wait_bytes(ref, sem):
        pltpu.make_async_copy(ref, ref, sem).wait()

    def send(src, dst, send_sem, recv_sem, p_, s_):
        pltpu.make_async_remote_copy(
            src_ref=src, dst_ref=dst, send_sem=send_sem, recv_sem=recv_sem,
            device_id=(p_, s_), device_id_type=MESH,
        ).start()

    span_peers = [lax.rem(col + d, ns) for d in range(1, ns)]
    row_peers = [lax.rem(row + d, np_) for d in range(1, np_)]
    y_peers = [lax.rem(row + CORES * d, np_) for d in range(1, rows_y)]

    loads = []
    for g in range(KVH):
        cols = pl.ds(g * HD, HD)
        for i, src in enumerate((k_ref, v_ref)):
            c = pltpu.make_async_copy(
                src.at[:, cols], kv[g].at[row, i], load_sem.at[g, i]
            )
            c.start()
            loads.append(c)
    line = lax.broadcasted_iota(jnp.int32, (prompts, HD), 0)
    pos_tile = jnp.zeros((prompts, HD), jnp.int32)
    for p in range(prompts):
        pos_tile = jnp.where(line == p, pos_in[0, p], pos_tile)
    pos_ref[...] = pos_tile
    len_ref[...] = jnp.full((XH, HD), len_in[0, 0], jnp.int32)
    pos_keep = pltpu.make_async_copy(pos_ref, pos_all.at[col], own_sem.at[1])
    pos_keep.start()
    len_keep = pltpu.make_async_copy(len_ref, len_all.at[row], own_sem.at[2])
    len_keep.start()

    barrier = pltpu.get_barrier_semaphore()
    for s in span_peers:
        pl.semaphore_signal(barrier, inc=1, device_id=(row, s), device_id_type=MESH)
    for r in row_peers:
        pl.semaphore_signal(barrier, inc=1, device_id=(r, col), device_id_type=MESH)
    pl.semaphore_wait(barrier, ns - 1 + np_ - 1)

    for r in row_peers:
        send(len_ref, len_all.at[row], len_send, len_recv, r, col)
    for s in span_peers:
        send(pos_ref, pos_all.at[col], pos_send, pos_recv, row, s)
    for g in range(KVH):
        loads[2 * g].wait()
        loads[2 * g + 1].wait()
        for r in y_peers:
            send(kv[g].at[row], kv[g].at[row], kvy_send.at[g], kvy_recv.at[g], r, col)
        send(kv[g].at[row], kv[g].at[row], kvp_send.at[g], kvp_recv.at[g], partner, col)

    for g in range(KVH):
        tiles = [
            q_in[:, (g * XH + x) * HD : (g * XH + x + 1) * HD].astype(jnp.float32)
            for x in range(XH)
        ]
        q_ref[g] = jnp.swapaxes(jnp.stack(tiles, axis=0), 0, 1).astype(jnp.bfloat16)
        for s in span_peers:
            send(q_ref.at[g], q_all.at[col, g], q_send.at[g], q_recv.at[g], row, s)

    q_keep = pltpu.make_async_copy(q_ref, q_all.at[col], own_sem.at[0])
    q_keep.start()
    for g in range(KVH):
        cols = slice(g * HD, (g + 1) * HD)
        fk_ref[g] = fk_in[:, cols].astype(jnp.float32)
        fv_ref[g] = fv_in[:, cols].astype(jnp.float32)

    lane = lax.broadcasted_iota(jnp.int32, (XH, HD), 1)
    own_ref[...] = jnp.zeros_like(own_ref)
    stat[...] = jnp.zeros_like(stat)

    def own_body(p, carry):
        tile = own_ref[...]
        for g in range(KVH):
            q8 = q_ref[g, p].astype(jnp.float32)
            dot = jnp.sum(q8 * fk_ref[g, pl.ds(p, 1), :], axis=1, keepdims=True)
            tile = jnp.where(lane == g * prompts + p, dot * (1.0 / math.sqrt(HD)), tile)
        own_ref[...] = tile
        return carry

    lax.fori_loop(0, prompts, own_body, 0)

    q_keep.wait()
    pos_keep.wait()
    len_keep.wait()
    wait_bytes(len_all.at[pl.ds(0, np_ - 1)], len_recv)
    wait_bytes(pos_all.at[pl.ds(0, ns - 1)], pos_recv)

    count = ns * XH
    slot_ids = lax.broadcasted_iota(jnp.int32, (count, slots), 1)
    lanes3 = lax.broadcasted_iota(jnp.int32, (ns, XH, HD), 2)
    start = col * slots
    step = 2 if prompts % 2 == 0 else 1

    for g in range(KVH):
        if rows_y > 1:
            wait_bytes(kv[g].at[pl.ds(0, rows_y - 1)], kvy_recv.at[g])
        for r in y_peers:
            send(kv[g].at[r], kv[g].at[r], kvp_send.at[g], kvp_recv.at[g], partner, col)
        wait_bytes(q_all.at[pl.ds(0, ns - 1), g], q_recv.at[g])
        wait_bytes(kv[g].at[pl.ds(0, rows_y)], kvp_recv.at[g])

        def one(p, g=g):
            o = owner_ref[0, p]
            q64 = q_all[:, g, p].astype(jnp.float32).reshape(count, HD).astype(jnp.bfloat16)
            keys = kv[g][o, 0]
            values = kv[g][o, 1]
            pos3 = jnp.broadcast_to(pos_all[:, pl.ds(p, 1), :], (ns, XH, HD))
            len3 = jnp.broadcast_to(len_all[o][None], (ns, XH, HD))
            limit = jnp.minimum(len3, pos3 - start).reshape(count, HD)
            limit = jnp.concatenate([limit] * (slots // HD), axis=1)
            visible = slot_ids < limit
            scores = lax.dot_general(
                q64, keys, (((1,), (1,)), ((), ())), preferred_element_type=jnp.float32
            ) * (1.0 / math.sqrt(HD))
            scores = jnp.where(visible, scores, NEGATIVE)
            top = jnp.max(scores, axis=1, keepdims=True)
            top = top.astype(jnp.bfloat16).astype(jnp.float32)
            weights = jnp.where(visible, jnp.exp(scores - top), 0.0)
            total = jnp.sum(weights, axis=1, keepdims=True)
            mix = jnp.dot(
                weights.astype(jnp.bfloat16), values, preferred_element_type=jnp.float32
            )
            part[:, g, p] = mix.reshape(ns, XH, HD).astype(jnp.bfloat16)
            here = lanes3 == g * prompts + p
            top3 = jnp.broadcast_to(top, (count, HD)).reshape(ns, XH, HD)
            total3 = jnp.broadcast_to(total, (count, HD)).reshape(ns, XH, HD)
            stat[:, 0] = jnp.where(here, top3, stat[:, 0])
            stat[:, 1] = jnp.where(here, total3, stat[:, 1])

        def body(i, carry):
            for k in range(step):
                one(i * step + k)
            return carry

        lax.fori_loop(0, prompts // step, body, 0)
        for s in span_peers:
            send(part.at[s, g], part_all.at[col, g], part_send.at[g], part_recv.at[g], row, s)
        pltpu.make_async_copy(part.at[col, g], part_all.at[col, g], keep_sem.at[g]).start()

    for s in span_peers:
        send(stat.at[s], stat_all.at[col], stat_send, stat_recv, row, s)
    pltpu.make_async_copy(stat.at[col], stat_all.at[col], own_sem.at[3]).start()

    wait_bytes(stat.at[col], own_sem.at[3])
    wait_bytes(stat_all.at[pl.ds(0, ns - 1)], stat_recv)
    tops = [stat_all[j, 0] for j in range(ns)]
    own = own_ref[...]
    high = own
    for t in tops:
        high = jnp.maximum(high, t)
    own_w = jnp.exp(own - high)
    factors = [jnp.exp(t - high) for t in tops]
    denom = own_w
    for j in range(ns):
        denom = denom + factors[j] * stat_all[j, 1]
    inv = 1.0 / denom
    for j in range(ns):
        stat_all[j, 0] = factors[j] * inv
    own_ref[...] = own_w * inv

    for g in range(KVH):
        wait_bytes(part.at[col, g], keep_sem.at[g])
        wait_bytes(part_all.at[pl.ds(0, ns - 1), g], part_recv.at[g])

    def combine(p, carry):
        shift = lax.rem(HD - p, HD)
        own_s = pltpu.roll(own_ref[...], shift, 1)
        sums = []
        for g in range(KVH):
            lo = g * prompts
            sums.append(own_s[:, lo : lo + 1] * fv_ref[g, pl.ds(p, 1), :])
        for j in range(ns):
            f = pltpu.roll(stat_all[j, 0], shift, 1)
            for g in range(KVH):
                lo = g * prompts
                sums[g] = sums[g] + f[:, lo : lo + 1] * part_all[j, g, p].astype(jnp.float32)
        for g in range(KVH):
            out_ref[p, g] = sums[g].astype(jnp.bfloat16)
        return carry

    lax.fori_loop(0, prompts, combine, 0)

    wait_bytes(len_all.at[pl.ds(0, np_ - 1)], len_send)
    wait_bytes(pos_all.at[pl.ds(0, ns - 1)], pos_send)
    wait_bytes(stat_all.at[pl.ds(0, ns - 1)], stat_send)
    for g in range(KVH):
        wait_bytes(q_all.at[pl.ds(0, ns - 1), g], q_send.at[g])
        if rows_y > 1:
            wait_bytes(kv[g].at[pl.ds(0, rows_y - 1)], kvy_send.at[g])
        wait_bytes(kv[g].at[pl.ds(0, rows_y)], kvp_send.at[g])
        wait_bytes(part_all.at[pl.ds(0, ns - 1), g], part_send.at[g])


def on_device(
    queries, query_pos, fresh_keys, fresh_values, cache_keys, cache_values, block_len, block_owner
):
    prompts = queries.shape[0]
    slots = cache_keys.shape[2]
    np_ = lax.axis_size("prompt")
    ns = lax.axis_size("span")
    vmem = pl.BlockSpec(memory_space=pltpu.VMEM)
    hbm = pl.BlockSpec(memory_space=pl.ANY)
    dma = pltpu.SemaphoreType.DMA
    bf16, f32, i32 = jnp.bfloat16, jnp.float32, jnp.int32
    out = pl.pallas_call(
        functools.partial(kernel, np_, ns, prompts, slots),
        out_shape=jax.ShapeDtypeStruct((prompts, KVH, XH, HD), bf16),
        in_specs=[pl.BlockSpec(memory_space=pltpu.SMEM)] * 3 + [vmem] * 3 + [hbm] * 2,
        out_specs=vmem,
        scratch_shapes=[
            pltpu.VMEM((KVH, prompts, XH, HD), bf16),
            pltpu.VMEM((prompts, HD), i32),
            pltpu.VMEM((XH, HD), i32),
            pltpu.VMEM((KVH, prompts, HD), f32),
            pltpu.VMEM((KVH, prompts, HD), f32),
            pltpu.VMEM((ns, KVH, prompts, XH, HD), bf16),
            pltpu.VMEM((ns, prompts, HD), i32),
            pltpu.VMEM((np_, XH, HD), i32),
            pltpu.VMEM((ns, KVH, prompts, XH, HD), bf16),
            pltpu.VMEM((ns, KVH, prompts, XH, HD), bf16),
            pltpu.VMEM((ns, 2, XH, HD), f32),
            pltpu.VMEM((ns, 2, XH, HD), f32),
            pltpu.VMEM((XH, HD), f32),
            dma((KVH,)), dma((KVH,)), dma, dma, dma, dma,
            dma((KVH, 2)), dma((KVH,)), dma((KVH,)), dma((KVH,)), dma((KVH,)),
            dma((KVH,)), dma((KVH,)), dma, dma, dma((KVH,)), dma((4,)),
        ]
        + [pltpu.VMEM((np_, 2, slots, HD), bf16)] * KVH,
        compiler_params=pltpu.CompilerParams(
            collective_id=0, has_side_effects=True, vmem_limit_bytes=60 * 1024 * 1024
        ),
    )(
        block_owner.reshape(1, prompts),
        query_pos.reshape(1, prompts),
        block_len,
        queries.reshape(prompts, H * HD),
        fresh_keys.reshape(prompts, KVH * HD),
        fresh_values.reshape(prompts, KVH * HD),
        cache_keys.reshape(slots, KVH * HD),
        cache_values.reshape(slots, KVH * HD),
    )
    return out.reshape(prompts, 1, H * HD)


def solution(mesh):
    return jax.shard_map(
        on_device,
        mesh=mesh,
        in_specs=(
            P("prompt", "span", None),
            P("prompt", "span"),
            P("prompt", "span", None),
            P("prompt", "span", None),
            P("prompt", "span", None, None),
            P("prompt", "span", None, None),
            P("prompt", "span"),
            P("span", "prompt", None),
        ),
        out_specs=P("prompt", "span", None),
        check_vma=False,
    )
```
